512 devices in a mesh: layer: 8 (over y_lo, core), row: 8 (over z), col: 8 (over y_hi, x).
Axes of the slice: x: 4, y: 8 (y_hi: 2, y_lo: 4; y = y_hi * 4 + y_lo), z: 8, core: 2. Of those that a mesh axis runs over, the one named last changes fastest.
Arguments:
- edge_weight: bfloat16 [8192, 8192], P('row', 'col'), may hold values from 0 to 1, as said below
Outputs:
- clustering: float32 [8, 1024], P('row', ('layer', 'col'))
The draws below stay inside these ranges and needn't reach their ends.
Inputs may be any that keep to these rules, and one draw needn't show every extreme that they name: `edge_weight`: symmetric with a zero diagonal; every vertex v is linked to v - 1 and v + 1 (modulo 8192); an edge's entry lies in [0.2, 1], all other entries are 0.
All inputs are finite; a program needn't handle non-finite values.
Results may differ from the reference program's by a relative error of at most 0.0003.
Values may be sent and summed in bfloat16 or wider, within the bound.
No kernel may reach another device: no remote copies, remote signals or barrier semaphores. Data moves between devices by JAX's collectives and lax.ppermute only.
A program may use at most 64 MiB of HBM per device.

```python
import jax
import jax.numpy as jnp
from jax import lax

VERTS = 8192
N_ROW = 8


def draw_edge_weight(key, part):
    keys = jax.random.split(jax.random.fold_in(key, 7), 4)
    index = jnp.arange(VERTS, dtype=jnp.float32)
    leaning = 0.25 * 4.0 ** (index / VERTS) * jax.random.uniform(keys[0], (VERTS,), minval=0.6, maxval=1.25)
    place = jax.random.uniform(keys[3], (VERTS,), minval=0.0, maxval=2.0 * jnp.pi)
    nearness = 0.5 + 0.5 * jnp.cos(place[:, None] - place[None, :])
    chance = jnp.sqrt(leaning[:, None] * leaning[None, :]) * (0.1 + 1.8 * nearness ** 4)
    coins = jax.random.uniform(keys[1], (VERTS, VERTS))
    first = jnp.arange(VERTS)[:, None]
    second = jnp.arange(VERTS)[None, :]
    upper = second > first
    linked = jnp.logical_and(coins < chance, upper)
    linked = jnp.logical_or(linked, linked.T)
    distance = jnp.abs(first - second)
    linked = jnp.logical_or(linked, jnp.logical_or(distance == 1, distance == VERTS - 1))
    values = jnp.exp(jax.random.uniform(keys[2], (VERTS, VERTS), minval=jnp.log(0.2), maxval=0.0))
    values = jnp.where(upper, values, 0.0)
    values = values + values.T
    return jnp.where(linked, values, 0.0).astype(jnp.float32).astype(jnp.bfloat16)


def setup_inputs(seed: int = 0) -> dict:
    arg_keys = jax.random.split(jax.random.key(seed), 2)
    edge_weight = draw_edge_weight(jax.random.fold_in(arg_keys[1], 71), 0)
    return {"edge_weight": edge_weight}


def reference(edge_weight):
    weights = edge_weight.astype(jnp.float32)
    order = jnp.arange(VERTS, dtype=jnp.int32)
    lower = jnp.where(order[:, None] > order[None, :], weights, jnp.zeros_like(weights))
    degree = jnp.sum(jnp.where(lower > 0, 1.0, 0.0).astype(jnp.float32), axis=1)
    span = VERTS // N_ROW

    def block_rows(index):
        rows = lax.dynamic_slice_in_dim(lower, index * span, span, 0)
        paths = jnp.dot(rows, lower, precision=lax.Precision.HIGHEST)
        return jnp.sum(paths * rows, axis=1)

    triangles = lax.map(block_rows, jnp.arange(N_ROW, dtype=jnp.int32)).reshape(VERTS)
    clustering = 2.0 * triangles / jnp.maximum(degree * (degree - 1.0), 2.0)
    return clustering.reshape(N_ROW, span)
```

```python
import functools

import jax
import jax.numpy as jnp
from jax import lax
from jax.experimental import pallas as pl
from jax.experimental.pallas import tpu as pltpu
from jax.sharding import PartitionSpec as P

F32 = jnp.float32
BLOCKS = 8
LABEL = [6, 0, 4, 2, 3, 5, 1, 7]
SLOPE = 5
DIAG_LAYER = [
    [3, 0, 7, 4, 6, 2, 1],
    [4, 6, 0, 2, 5, 3, 7],
    [5, 1, 4, 0, 2, 6, 3],
    [2, 1, 7, 4, 0, 6, 3],
    [0, 3, 4, 6, 7, 5, 2],
    [4, 7, 0, 2, 6, 3, 1],
    [3, 6, 1, 5, 0, 4, 2],
    [6, 2, 4, 1, 5, 0, 7],
]
ROWS_KIND, COLS_KIND, THIRD_KIND = 1, 2, 3
OWN_ROW, OWN_COL, OWN_DIAG = 1, 2, 3


def times(a, b):
    r = 0
    for i in range(3):
        if (b >> i) & 1:
            r ^= a << i
    for i in (4, 3):
        if (r >> i) & 1:
            r ^= 0b1011 << (i - 3)
    return r


def third_block(r, c):
    return LABEL.index(times(SLOPE, LABEL[r]) ^ times(SLOPE ^ 1, LABEL[c]))


def node(r, c):
    return r * BLOCKS + c


def device(layer, r, c):
    return layer * BLOCKS * BLOCKS + node(r, c)


def plan():
    col_pairs, row_pairs, kinds = [], [], [[0, 0]] * (BLOCKS * BLOCKS)
    for r in range(BLOCKS):
        for c in range(BLOCKS):
            if r == c:
                continue
            m = third_block(r, c)
            col_pairs.append((node(r, m), node(r, c)))
            row_pairs.append((node(m, c), node(r, c)))
            top = max(r, c, m)
            kinds[node(r, c)] = [{r: ROWS_KIND, c: COLS_KIND, m: THIRD_KIND}[top], top]
    diag_pairs, own = [], [0] * (BLOCKS**3)
    for d in range(BLOCKS):
        for layer in range(BLOCKS):
            own[device(layer, d, d)] = OWN_DIAG
        others = [o for o in range(BLOCKS) if o != d]
        for o, layer in zip(others, DIAG_LAYER[d]):
            target = device(layer, max(d, o), min(d, o))
            diag_pairs.append((device(layer, d, d), target))
            own[target] = OWN_COL if o > d else OWN_ROW
    return col_pairs, row_pairs, diag_pairs, kinds, own


def mm(a, b, dims=((1,), (0,))):
    return lax.dot_general(a, b, (dims, ((), ())), preferred_element_type=F32)


def fold_lanes(w):
    part = w[:, :128]
    for t in range(1, w.shape[1] // 128):
        part = part + w[:, 128 * t : 128 * (t + 1)]
    return jnp.sum(part.T, axis=0, keepdims=True)


def fold_rows(w):
    return jnp.sum(w.reshape(w.shape[0] // 8, 8, w.shape[1]), axis=0)


STEP = 256


def triple_kernel(info_ref, b_ref, x_ref, z_ref, out_ref):
    kind, top, layer = info_ref[0], info_ref[1], info_ref[2]
    n = b_ref.shape[0]
    out_ref[...] = jnp.zeros_like(out_ref)

    def put(vector, start):
        shape = (out_ref.shape[0], vector.shape[1])
        row = lax.broadcasted_iota(jnp.int32, shape, 0)
        spread = jnp.broadcast_to(vector, shape)
        out_ref[:, start : start + shape[1]] = jnp.where(row == top, spread, jnp.zeros_like(spread))

    @pl.when(kind == ROWS_KIND)
    def _():
        for s in range(0, n, STEP):
            w = mm(x_ref[s : s + STEP, :], z_ref[...]) * b_ref[s : s + STEP, :].astype(F32)
            put(fold_lanes(w), s)

    @pl.when(kind == COLS_KIND)
    def _():
        acc = jnp.zeros((8, n), F32)
        for s in range(0, n, STEP):
            w = mm(x_ref[s : s + STEP, :], z_ref[...]) * b_ref[s : s + STEP, :].astype(F32)
            acc = acc + fold_rows(w)
        put(jnp.sum(acc, axis=0, keepdims=True), 0)

    @pl.when(kind == THIRD_KIND)
    def _():
        width = x_ref.shape[1]
        acc = jnp.zeros((8, width), F32)
        for s in range(0, n, STEP):
            q = mm(b_ref[s : s + STEP, :], z_ref[...], ((1,), (1,)))
            acc = acc + fold_rows(q * x_ref[s : s + STEP, :].astype(F32))
        total = jnp.sum(acc, axis=0, keepdims=True)
        for k in range(n // width):
            @pl.when(layer == k)
            def _(k=k):
                put(total, k * width)


def own_kernel(info_ref, b_ref, u_ref, out_ref):
    own, layer, side = info_ref[0], info_ref[1], info_ref[2]
    n = b_ref.shape[0]
    h = n // 2
    width = n // BLOCKS
    out_ref[...] = jnp.zeros_like(out_ref)
    zero = jnp.zeros((), u_ref.dtype)

    def below(w, first_row):
        row = lax.broadcasted_iota(jnp.int32, w.shape, 0) + first_row
        col = lax.broadcasted_iota(jnp.int32, w.shape, 1)
        return jnp.where(row > col, w, jnp.zeros((), w.dtype))

    def halves():
        mix = u_ref[:, h:]
        row = lax.broadcasted_iota(jnp.int32, mix.shape, 0)
        col = lax.broadcasted_iota(jnp.int32, mix.shape, 1)
        return u_ref[:, :h], jnp.where(row < col, mix, zero), jnp.where(row > col, mix, zero)

    @pl.when(own == OWN_COL)
    def _():
        across, first, second = halves()
        for s in range(0, n, STEP):
            lo, hi = b_ref[s : s + STEP, :h], b_ref[s : s + STEP, h:]
            p_lo = mm(hi, across) + mm(lo, first)
            w = p_lo * lo.astype(F32) + mm(hi, second) * hi.astype(F32)
            out_ref[0:1, s : s + STEP] = fold_lanes(w)

    @pl.when(own == OWN_ROW)
    def _():
        across, first, second = halves()
        for s in range(0, h, STEP):
            p = mm(first[:, s : s + STEP], b_ref[:h, :], ((0,), (0,)))
            out_ref[0:1, s : s + STEP] = fold_lanes(p * b_ref[s : s + STEP, :].astype(F32))
        for s in range(0, h, STEP):
            p = mm(across[s : s + STEP, :], b_ref[:h, :]) + mm(second[s : s + STEP, :], b_ref[h:, :])
            out_ref[0:1, h + s : h + s + STEP] = fold_lanes(p * b_ref[h + s : h + s + STEP, :].astype(F32))

    for k in range(BLOCKS):
        cut = slice(k * width, (k + 1) * width)

        @pl.when(jnp.logical_and(layer == k, side >= 0))
        def _(cut=cut, k=k):
            rows = b_ref[cut, :]
            row = lax.broadcasted_iota(jnp.int32, rows.shape, 0) + k * width
            col = lax.broadcasted_iota(jnp.int32, rows.shape, 1)
            mine = jnp.logical_and(rows.astype(F32) > 0, jnp.logical_or(side > 0, row > col))
            out_ref[1:2, cut] = fold_lanes(jnp.where(mine, 1.0, 0.0).astype(F32))

        @pl.when(jnp.logical_and(layer == k, own == OWN_DIAG))
        def _(cut=cut, k=k):
            middle = below(b_ref[cut, :], k * width)
            for s in range(0, n, STEP):
                mine = below(b_ref[s : s + STEP, :], s)
                w = mm(mine[:, cut], middle) * mine.astype(F32)
                out_ref[0:1, s : s + STEP] = fold_lanes(w)


def vmem_call(kernel, out_shape, flops, nbytes, name):
    whole = pl.BlockSpec(memory_space=pltpu.VMEM)

    def call(info, *arrays):
        return pl.pallas_call(
            kernel,
            out_shape=out_shape,
            in_specs=[pl.BlockSpec(memory_space=pltpu.SMEM)] + [whole] * len(arrays),
            out_specs=whole,
            name=name,
            cost_estimate=pl.CostEstimate(flops=flops, bytes_accessed=nbytes, transcendentals=0),
            compiler_params=pltpu.CompilerParams(vmem_limit_bytes=32 * 1024 * 1024),
        )(info, *arrays)

    return call


def local(edge_weight):
    n = edge_weight.shape[0]
    width, half = n // BLOCKS, n // 2
    col_pairs, row_pairs, diag_pairs, kinds, own = plan()
    layer, r, c = (lax.axis_index(name).astype(jnp.int32) for name in ("layer", "row", "col"))
    here = r * BLOCKS + c
    kind = lax.dynamic_slice_in_dim(jnp.array(kinds, jnp.int32).reshape(-1), 2 * here, 2)
    own_kind = lax.dynamic_slice_in_dim(jnp.array(own, jnp.int32), layer * BLOCKS * BLOCKS + here, 1)
    triple_info = jnp.concatenate([kind, layer[None]])
    own_info = jnp.concatenate([own_kind, layer[None], (r - c)[None]])

    columns = lax.dynamic_slice_in_dim(edge_weight, layer * width, width, 1)
    rows = lax.dynamic_slice_in_dim(edge_weight, layer * width, width, 0)
    k = jnp.arange(half, dtype=jnp.int32)
    mix = jnp.where(k[:, None] > k[None, :], edge_weight[half:, half:], edge_weight[:half, :half])
    packed = jnp.concatenate([edge_weight[half:, :half], mix], axis=1)

    x = lax.ppermute(columns, ("row", "col"), col_pairs)
    z = lax.ppermute(rows, ("row", "col"), row_pairs)
    u = lax.ppermute(packed, ("layer", "row", "col"), diag_pairs)

    triples = vmem_call(
        triple_kernel, jax.ShapeDtypeStruct((BLOCKS, n), F32), 2 * n * n * width, 2 * n * n, "triples"
    )(triple_info, edge_weight, x, z)
    back = lax.all_to_all(triples, "row", 0, 0, tiled=True)
    mine = vmem_call(
        own_kernel, jax.ShapeDtypeStruct((2, n), F32), 3 * n * n * half, 4 * n * n, "own"
    )(own_info, edge_weight, u)
    total = jnp.sum(back, axis=0) + mine[0]
    peers = BLOCKS * BLOCKS
    sent = jnp.stack([total.reshape(peers, n // peers), mine[1].reshape(peers, n // peers)], axis=1)
    got = jnp.sum(lax.all_to_all(sent, ("layer", "col"), 0, 0, tiled=True), axis=0)
    degree = got[1]
    clustering = 2.0 * got[0] / jnp.maximum(degree * (degree - 1.0), 2.0)
    return clustering.reshape(1, -1)


def solution(mesh):
    placed = (P("row", "col"),)
    return jax.shard_map(
        local, mesh=mesh, in_specs=placed, out_specs=P("row", ("layer", "col")), check_vma=False
    )
```

```python
import jax
import jax.numpy as jnp
from jax import lax
from jax.experimental import pallas as pl
from jax.experimental.pallas import tpu as pltpu
from jax.sharding import PartitionSpec as P


F32 = jnp.float32
BLOCKS = 8
THIRD = [
    [0, 4, 3, 7, 2, 6, 1, 5],
    [2, 1, 7, 6, 3, 0, 5, 4],
    [6, 5, 2, 1, 7, 4, 3, 0],
    [4, 0, 5, 3, 6, 1, 7, 2],
    [5, 6, 1, 2, 4, 7, 0, 3],
    [3, 7, 0, 4, 1, 5, 2, 6],
    [7, 2, 4, 0, 5, 3, 6, 1],
    [1, 3, 6, 5, 0, 2, 4, 7],
]
DIAG_LAYER = [
    [3, 0, 7, 4, 6, 2, 1],
    [4, 6, 0, 2, 5, 3, 7],
    [5, 1, 4, 0, 2, 6, 3],
    [2, 1, 7, 4, 0, 6, 3],
    [0, 3, 4, 6, 7, 5, 2],
    [4, 7, 0, 2, 6, 3, 1],
    [3, 6, 1, 5, 0, 4, 2],
    [6, 2, 4, 1, 5, 0, 7],
]
ROWS_KIND, COLS_KIND, THIRD_KIND = 1, 2, 3
OWN_ROW, OWN_COL, OWN_DIAG = 1, 2, 3


def node(r, c):
    return r * BLOCKS + c


def device(layer, r, c):
    return layer * BLOCKS * BLOCKS + node(r, c)


def plan():
    col_pairs, row_pairs, kinds = [], [], [[0, 0]] * (BLOCKS * BLOCKS)
    for r in range(BLOCKS):
        for c in range(BLOCKS):
            if r == c:
                continue
            m = THIRD[r][c]
            col_pairs.append((node(r, m), node(r, c)))
            row_pairs.append((node(m, c), node(r, c)))
            top = max(r, c, m)
            kinds[node(r, c)] = [{r: ROWS_KIND, c: COLS_KIND, m: THIRD_KIND}[top], top]
    diag_pairs, own = [], [0] * (BLOCKS**3)
    for d in range(BLOCKS):
        for layer in range(BLOCKS):
            own[device(layer, d, d)] = OWN_DIAG
        others = [o for o in range(BLOCKS) if o != d]
        for o, layer in zip(others, DIAG_LAYER[d]):
            target = device(layer, max(d, o), min(d, o))
            diag_pairs.append((device(layer, d, d), target))
            own[target] = OWN_COL if o > d else OWN_ROW
    return col_pairs, row_pairs, diag_pairs, kinds, own


def mm(a, b, dims=((1,), (0,))):
    return lax.dot_general(a, b, (dims, ((), ())), preferred_element_type=F32)


def fold_lanes(w):
    part = w[:, :128]
    for t in range(1, w.shape[1] // 128):
        part = part + w[:, 128 * t : 128 * (t + 1)]
    return jnp.sum(part.T, axis=0, keepdims=True)


def fold_rows(w):
    return jnp.sum(w.reshape(w.shape[0] // 8, 8, w.shape[1]), axis=0)


STEP = 256


def triple_kernel(info_ref, b_ref, x_ref, z_ref, out_ref):
    here = lax.axis_index("row") * BLOCKS + lax.axis_index("col")
    kind, top, layer = info_ref[2 * here], info_ref[2 * here + 1], lax.axis_index("layer")
    n = b_ref.shape[0]
    out_ref[...] = jnp.zeros_like(out_ref)

    def put(vector, start):
        shape = (out_ref.shape[0], vector.shape[1])
        row = lax.broadcasted_iota(jnp.int32, shape, 0)
        spread = jnp.broadcast_to(vector, shape)
        out_ref[:, start : start + shape[1]] = jnp.where(row == top, spread, jnp.zeros_like(spread))

    @pl.when(kind == ROWS_KIND)
    def _():
        for s in range(0, n, STEP):
            w = mm(x_ref[s : s + STEP, :], z_ref[...]) * b_ref[s : s + STEP, :].astype(F32)
            put(fold_lanes(w), s)

    @pl.when(kind == COLS_KIND)
    def _():
        acc = jnp.zeros((8, n), F32)
        for s in range(0, n, STEP):
            w = mm(x_ref[s : s + STEP, :], z_ref[...]) * b_ref[s : s + STEP, :].astype(F32)
            acc = acc + fold_rows(w)
        put(jnp.sum(acc, axis=0, keepdims=True), 0)

    @pl.when(kind == THIRD_KIND)
    def _():
        width = x_ref.shape[1]
        acc = jnp.zeros((8, width), F32)
        for s in range(0, n, STEP):
            q = mm(b_ref[s : s + STEP, :], z_ref[...], ((1,), (1,)))
            acc = acc + fold_rows(q * x_ref[s : s + STEP, :].astype(F32))
        total = jnp.sum(acc, axis=0, keepdims=True)
        for k in range(n // width):
            @pl.when(layer == k)
            def _(k=k):
                put(total, k * width)


def own_kernel(info_ref, b_ref, u_ref, out_ref):
    layer, r, c = (lax.axis_index(name) for name in ("layer", "row", "col"))
    own, side = info_ref[(layer * BLOCKS + r) * BLOCKS + c], r - c
    n = b_ref.shape[0]
    h = n // 2
    width = n // BLOCKS
    out_ref[...] = jnp.zeros_like(out_ref)
    zero = jnp.zeros((), u_ref.dtype)

    def below(w, first_row):
        row = lax.broadcasted_iota(jnp.int32, w.shape, 0) + first_row
        col = lax.broadcasted_iota(jnp.int32, w.shape, 1)
        return jnp.where(row > col, w, jnp.zeros((), w.dtype))

    def halves():
        mix = u_ref[:, h:]
        row = lax.broadcasted_iota(jnp.int32, mix.shape, 0)
        col = lax.broadcasted_iota(jnp.int32, mix.shape, 1)
        return u_ref[:, :h], jnp.where(row < col, mix, zero), jnp.where(row > col, mix, zero)

    @pl.when(own == OWN_COL)
    def _():
        across, first, second = halves()
        for s in range(0, n, STEP):
            lo, hi = b_ref[s : s + STEP, :h], b_ref[s : s + STEP, h:]
            p_lo = mm(hi, across) + mm(lo, first)
            w = p_lo * lo.astype(F32) + mm(hi, second) * hi.astype(F32)
            out_ref[0:1, s : s + STEP] = fold_lanes(w)

    @pl.when(own == OWN_ROW)
    def _():
        across, first, second = halves()
        for s in range(0, h, STEP):
            p = mm(first[:, s : s + STEP], b_ref[:h, :], ((0,), (0,)))
            out_ref[0:1, s : s + STEP] = fold_lanes(p * b_ref[s : s + STEP, :].astype(F32))
        for s in range(0, h, STEP):
            p = mm(across[s : s + STEP, :], b_ref[:h, :]) + mm(second[s : s + STEP, :], b_ref[h:, :])
            out_ref[0:1, h + s : h + s + STEP] = fold_lanes(p * b_ref[h + s : h + s + STEP, :].astype(F32))

    for k in range(BLOCKS):
        cut = slice(k * width, (k + 1) * width)

        @pl.when(jnp.logical_and(layer == k, side >= 0))
        def _(cut=cut, k=k):
            rows = b_ref[cut, :]
            row = lax.broadcasted_iota(jnp.int32, rows.shape, 0) + k * width
            col = lax.broadcasted_iota(jnp.int32, rows.shape, 1)
            mine = jnp.logical_and(rows.astype(F32) > 0, jnp.logical_or(side > 0, row > col))
            out_ref[1:2, cut] = fold_lanes(jnp.where(mine, 1.0, 0.0).astype(F32))

        @pl.when(jnp.logical_and(layer == k, own == OWN_DIAG))
        def _(cut=cut, k=k):
            middle = below(b_ref[cut, :], k * width)
            for s in range(0, n, STEP):
                mine = below(b_ref[s : s + STEP, :], s)
                w = mm(mine[:, cut], middle) * mine.astype(F32)
                out_ref[0:1, s : s + STEP] = fold_lanes(w)


def vmem_call(kernel, out_shape, flops, nbytes):
    whole = pl.BlockSpec(memory_space=pltpu.VMEM)

    def call(info, *arrays):
        return pl.pallas_call(
            kernel,
            out_shape=out_shape,
            in_specs=[pl.BlockSpec(memory_space=pltpu.SMEM)] + [whole] * len(arrays),
            out_specs=whole,
            cost_estimate=pl.CostEstimate(flops=flops, bytes_accessed=nbytes, transcendentals=0),
            compiler_params=pltpu.CompilerParams(vmem_limit_bytes=32 * 1024 * 1024),
        )(info, *arrays)

    return call


def step(edge_weight):
    n = edge_weight.shape[0]
    width, half = n // BLOCKS, n // 2
    col_pairs, row_pairs, diag_pairs, kinds, own = plan()
    layer = lax.axis_index("layer")
    triple_info = jnp.array(kinds, jnp.int32).reshape(-1)
    own_info = jnp.array(own, jnp.int32)

    columns = lax.dynamic_slice_in_dim(edge_weight, layer * width, width, 1)
    rows = lax.dynamic_slice_in_dim(edge_weight, layer * width, width, 0)
    x = lax.ppermute(columns, ("row", "col"), col_pairs)
    z = lax.ppermute(rows, ("row", "col"), row_pairs)
    k = jnp.arange(half, dtype=jnp.int32)
    mix = jnp.where(k[:, None] > k[None, :], edge_weight[half:, half:], edge_weight[:half, :half])
    packed = jnp.concatenate([edge_weight[half:, :half], mix], axis=1)
    u = lax.ppermute(packed, ("layer", "row", "col"), diag_pairs)

    triples = vmem_call(
        triple_kernel, jax.ShapeDtypeStruct((BLOCKS, n), F32), 2 * n * n * width, 2 * n * n
    )(triple_info, edge_weight, x, z)
    back = lax.all_to_all(triples, "row", 0, 0, tiled=True)
    mine = vmem_call(
        own_kernel, jax.ShapeDtypeStruct((2, n), F32), 3 * n * n * half, 4 * n * n
    )(own_info, edge_weight, u)
    total = jnp.sum(back, axis=0) + mine[0]
    peers = BLOCKS * BLOCKS
    sent = jnp.stack([total.reshape(peers, n // peers), mine[1].reshape(peers, n // peers)], axis=1)
    got = jnp.sum(lax.all_to_all(sent, ("layer", "col"), 0, 0, tiled=True), axis=0)
    degree = got[1]
    clustering = 2.0 * got[0] / jnp.maximum(degree * (degree - 1.0), 2.0)
    return clustering.reshape(1, -1)


def solution(mesh):
    placed = (P("row", "col"),)
    return jax.shard_map(
        step, mesh=mesh, in_specs=placed, out_specs=P("row", ("layer", "col")), check_vma=False
    )
```

```python
import jax
import jax.numpy as jnp
from jax import lax
from jax.experimental import pallas as pl
from jax.experimental.pallas import tpu as pltpu
from jax.sharding import PartitionSpec as P


F32 = jnp.float32
BLOCKS = 8
THIRD = [
    [0, 3, 6, 4, 2, 7, 5, 1],
    [4, 1, 0, 5, 3, 6, 7, 2],
    [5, 6, 2, 1, 7, 4, 3, 0],
    [2, 7, 5, 3, 6, 0, 1, 4],
    [7, 5, 1, 2, 4, 3, 0, 6],
    [1, 2, 7, 6, 0, 5, 4, 3],
    [3, 0, 4, 7, 1, 2, 6, 5],
    [6, 4, 3, 0, 5, 1, 2, 7],
]
PACKED_LAYER = [
    [-1, 5, 2, 6, 1, 3, 7, 4],
    [3, -1, 4, 1, 6, 2, 7, 5],
    [6, 0, -1, 1, 2, 4, 7, 3],
    [1, 6, 5, -1, 0, 7, 4, 2],
    [-1, -1, 5, 1, -1, 0, 6, 3],
    [-1, 7, -1, 0, 5, -1, 6, 1],
    [-1, 4, 1, -1, 7, 0, -1, 2],
    [-1, 1, 6, -1, 4, 7, 0, -1],
]
GRAM_LAYERS = {
    (4, 0): (1, 4),
    (4, 1): (3, 7),
    (5, 0): (2, 4),
    (5, 2): (0, 5),
    (6, 0): (1, 4),
    (6, 3): (3, 7),
    (7, 0): (3, 5),
    (7, 3): (0, 6),
}
ROWS_KIND, COLS_KIND, THIRD_KIND = 1, 2, 3
OWN_ROW, OWN_COL, OWN_DIAG, OWN_GRAM = 1, 2, 3, 4


def node(r, c):
    return r * BLOCKS + c


def device(layer, r, c):
    return layer * BLOCKS * BLOCKS + node(r, c)


def plan():
    col_pairs, row_pairs, kinds = [], [], [[0, 0]] * (BLOCKS * BLOCKS)
    for r in range(BLOCKS):
        for c in range(BLOCKS):
            if r == c:
                continue
            m = THIRD[r][c]
            col_pairs.append((node(r, m), node(r, c)))
            row_pairs.append((node(m, c), node(r, c)))
            top = max(r, c, m)
            kinds[node(r, c)] = [{r: ROWS_KIND, c: COLS_KIND, m: THIRD_KIND}[top], top]
    diag_pairs, own = [], [0] * (BLOCKS**3)
    for d in range(BLOCKS):
        for layer in range(BLOCKS):
            own[device(layer, d, d)] = OWN_DIAG
        for o in range(BLOCKS):
            layer = PACKED_LAYER[d][o]
            if layer >= 0:
                target = device(layer, max(d, o), min(d, o))
                diag_pairs.append((device(layer, d, d), target))
                own[target] = OWN_COL if o > d else OWN_ROW
            for layer in GRAM_LAYERS.get((d, o), ()):
                target = device(layer, d, d)
                diag_pairs.append((device(layer, o, d), target))
                own[target] = OWN_GRAM
    return col_pairs, row_pairs, diag_pairs, kinds, own


def mm(a, b, dims=((1,), (0,))):
    return lax.dot_general(a, b, (dims, ((), ())), preferred_element_type=F32)


def fold_lanes(w):
    part = w[:, :128]
    for t in range(1, w.shape[1] // 128):
        part = part + w[:, 128 * t : 128 * (t + 1)]
    return jnp.sum(part.T, axis=0, keepdims=True)


def fold_rows(w):
    return jnp.sum(w.reshape(w.shape[0] // 8, 8, w.shape[1]), axis=0)


STEP = 256


def triple_kernel(info_ref, b_ref, x_ref, z_ref, out_ref):
    here = lax.axis_index("row") * BLOCKS + lax.axis_index("col")
    kind, top, layer = info_ref[2 * here], info_ref[2 * here + 1], lax.axis_index("layer")
    n = b_ref.shape[0]
    out_ref[...] = jnp.zeros_like(out_ref)

    def put(vector, start):
        shape = (out_ref.shape[0], vector.shape[1])
        row = lax.broadcasted_iota(jnp.int32, shape, 0)
        spread = jnp.broadcast_to(vector, shape)
        out_ref[:, start : start + shape[1]] = jnp.where(row == top, spread, jnp.zeros_like(spread))

    @pl.when(kind == ROWS_KIND)
    def _():
        for s in range(0, n, STEP):
            w = mm(x_ref[s : s + STEP, :], z_ref[...]) * b_ref[s : s + STEP, :].astype(F32)
            put(fold_lanes(w), s)

    @pl.when(kind == COLS_KIND)
    def _():
        acc = jnp.zeros((8, n), F32)
        for s in range(0, n, STEP):
            w = mm(x_ref[s : s + STEP, :], z_ref[...]) * b_ref[s : s + STEP, :].astype(F32)
            acc = acc + fold_rows(w)
        put(jnp.sum(acc, axis=0, keepdims=True), 0)

    @pl.when(kind == THIRD_KIND)
    def _():
        width = x_ref.shape[1]
        acc = jnp.zeros((8, width), F32)
        for s in range(0, n, STEP):
            q = mm(b_ref[s : s + STEP, :], z_ref[...], ((1,), (1,)))
            acc = acc + fold_rows(q * x_ref[s : s + STEP, :].astype(F32))
        total = jnp.sum(acc, axis=0, keepdims=True)
        for k in range(n // width):
            @pl.when(layer == k)
            def _(k=k):
                put(total, k * width)


def own_kernel(info_ref, b_ref, u_ref, out_ref):
    layer, r, c = (lax.axis_index(name) for name in ("layer", "row", "col"))
    own, side = info_ref[(layer * BLOCKS + r) * BLOCKS + c], r - c
    n = b_ref.shape[0]
    h = n // 2
    width = n // BLOCKS
    out_ref[...] = jnp.zeros_like(out_ref)
    zero = jnp.zeros((), u_ref.dtype)

    def below(w, first_row):
        row = lax.broadcasted_iota(jnp.int32, w.shape, 0) + first_row
        col = lax.broadcasted_iota(jnp.int32, w.shape, 1)
        return jnp.where(row > col, w, jnp.zeros((), w.dtype))

    def halves():
        mix = u_ref[:, h:]
        row = lax.broadcasted_iota(jnp.int32, mix.shape, 0)
        col = lax.broadcasted_iota(jnp.int32, mix.shape, 1)
        return u_ref[:, :h], jnp.where(row < col, mix, zero), jnp.where(row > col, mix, zero)

    @pl.when(own == OWN_COL)
    def _():
        across, first, second = halves()
        for s in range(0, n, STEP):
            lo, hi = b_ref[s : s + STEP, :h], b_ref[s : s + STEP, h:]
            p_lo = mm(hi, across) + mm(lo, first)
            w = p_lo * lo.astype(F32) + mm(hi, second) * hi.astype(F32)
            out_ref[0:1, s : s + STEP] = fold_lanes(w)

    @pl.when(own == OWN_ROW)
    def _():
        across, first, second = halves()
        for s in range(0, h, STEP):
            p = mm(first[:, s : s + STEP], b_ref[:h, :], ((0,), (0,)))
            out_ref[0:1, s : s + STEP] = fold_lanes(p * b_ref[s : s + STEP, :].astype(F32))
        for s in range(0, h, STEP):
            p = mm(across[s : s + STEP, :], b_ref[:h, :]) + mm(second[s : s + STEP, :], b_ref[h:, :])
            out_ref[0:1, h + s : h + s + STEP] = fold_lanes(p * b_ref[h + s : h + s + STEP, :].astype(F32))

    for k in range(BLOCKS):
        cut = slice(k * width, (k + 1) * width)

        @pl.when(jnp.logical_and(layer == k, side >= 0))
        def _(cut=cut, k=k):
            rows = b_ref[cut, :]
            row = lax.broadcasted_iota(jnp.int32, rows.shape, 0) + k * width
            col = lax.broadcasted_iota(jnp.int32, rows.shape, 1)
            mine = jnp.logical_and(rows.astype(F32) > 0, jnp.logical_or(side > 0, row > col))
            out_ref[1:2, cut] = fold_lanes(jnp.where(mine, 1.0, 0.0).astype(F32))

        @pl.when(jnp.logical_and(layer == k, side == 0))
        def _(cut=cut, k=k):
            middle = below(b_ref[cut, :], k * width)
            for s in range(0, n, STEP):
                mine = below(b_ref[s : s + STEP, :], s)
                w = mm(mine[:, cut], middle) * mine.astype(F32)
                out_ref[0:1, s : s + STEP] = fold_lanes(w)


    @pl.when(own == OWN_GRAM)
    def _():
        for s in range(0, n, STEP):
            e = s + STEP
            g = mm(u_ref[:, s:e], u_ref[:, :e], ((0,), (0,)))
            out_ref[0:1, s:e] += fold_lanes(g * below(b_ref[s:e, :e], s).astype(F32))


def cut_kernel(b_ref, columns_ref, rows_ref, sems):
    width = columns_ref.shape[1]
    start = pl.multiple_of(lax.axis_index("layer") * width, width)
    copies = (
        pltpu.make_async_copy(b_ref.at[:, pl.ds(start, width)], columns_ref, sems.at[0]),
        pltpu.make_async_copy(b_ref.at[pl.ds(start, width), :], rows_ref, sems.at[1]),
    )
    for copy in copies:
        copy.start()
    for copy in copies:
        copy.wait()


def pack_kernel(b_ref, out_ref):
    h = out_ref.shape[0]
    diagonal = lax.axis_index("row") == lax.axis_index("col")
    second = lax.axis_index("layer") >= BLOCKS // 2

    @pl.when(diagonal)
    def _():
        out_ref[:, :h] = b_ref[h:, :h]
        row = lax.broadcasted_iota(jnp.int32, (h, h), 0)
        col = lax.broadcasted_iota(jnp.int32, (h, h), 1)
        out_ref[:, h:] = jnp.where(row > col, b_ref[h:, h:], b_ref[:h, :h])

    @pl.when(jnp.logical_not(diagonal))
    def _():
        @pl.when(second)
        def _():
            out_ref[...] = b_ref[h:, :]

        @pl.when(jnp.logical_not(second))
        def _():
            out_ref[...] = b_ref[:h, :]


def cut(edge_weight):
    n = edge_weight.shape[0]
    width = n // BLOCKS
    return pl.pallas_call(
        cut_kernel,
        out_shape=(
            jax.ShapeDtypeStruct((n, width), edge_weight.dtype),
            jax.ShapeDtypeStruct((width, n), edge_weight.dtype),
        ),
        in_specs=[pl.BlockSpec(memory_space=pltpu.HBM)],
        out_specs=(pl.BlockSpec(memory_space=pltpu.VMEM), pl.BlockSpec(memory_space=pltpu.VMEM)),
        scratch_shapes=[pltpu.SemaphoreType.DMA((2,))],
        name="cut",
        cost_estimate=pl.CostEstimate(flops=0, bytes_accessed=4 * n * width, transcendentals=0),
        compiler_params=pltpu.CompilerParams(vmem_limit_bytes=8 * 1024 * 1024),
    )(edge_weight)


def pack(edge_weight):
    n = edge_weight.shape[0]
    whole = pl.BlockSpec(memory_space=pltpu.VMEM)
    return pl.pallas_call(
        pack_kernel,
        out_shape=jax.ShapeDtypeStruct((n // 2, n), edge_weight.dtype),
        in_specs=[whole],
        out_specs=whole,
        name="pack",
        cost_estimate=pl.CostEstimate(flops=0, bytes_accessed=2 * n * n, transcendentals=0),
        compiler_params=pltpu.CompilerParams(vmem_limit_bytes=16 * 1024 * 1024),
    )(edge_weight)


def vmem_call(kernel, out_shape, flops, nbytes):
    whole = pl.BlockSpec(memory_space=pltpu.VMEM)

    def call(info, *arrays):
        return pl.pallas_call(
            kernel,
            out_shape=out_shape,
            in_specs=[pl.BlockSpec(memory_space=pltpu.SMEM)] + [whole] * len(arrays),
            out_specs=whole,
            cost_estimate=pl.CostEstimate(flops=flops, bytes_accessed=nbytes, transcendentals=0),
            compiler_params=pltpu.CompilerParams(vmem_limit_bytes=32 * 1024 * 1024),
        )(info, *arrays)

    return call


def step(edge_weight):
    n = edge_weight.shape[0]
    width, half = n // BLOCKS, n // 2
    col_pairs, row_pairs, diag_pairs, kinds, own = plan()
    triple_info = jnp.array(kinds, jnp.int32).reshape(-1)
    own_info = jnp.array(own, jnp.int32)

    columns, rows = cut(edge_weight)
    x = lax.ppermute(columns, ("row", "col"), col_pairs)
    z = lax.ppermute(rows, ("row", "col"), row_pairs)
    packed = pack(edge_weight)
    u = lax.ppermute(packed, ("layer", "row", "col"), diag_pairs)

    triples = vmem_call(
        triple_kernel, jax.ShapeDtypeStruct((BLOCKS, n), F32), 2 * n * n * width, 2 * n * n
    )(triple_info, edge_weight, x, z)
    back = lax.all_to_all(triples, "row", 0, 0, tiled=True)
    mine = vmem_call(
        own_kernel, jax.ShapeDtypeStruct((2, n), F32), 3 * n * n * half, 4 * n * n
    )(own_info, edge_weight, u)
    total = jnp.sum(back, axis=0) + mine[0]
    peers = BLOCKS * BLOCKS
    sent = jnp.stack([total.reshape(peers, n // peers), mine[1].reshape(peers, n // peers)], axis=1)
    got = jnp.sum(lax.all_to_all(sent, ("layer", "col"), 0, 0, tiled=True), axis=0)
    degree = got[1]
    clustering = 2.0 * got[0] / jnp.maximum(degree * (degree - 1.0), 2.0)
    return clustering.reshape(1, -1)


def solution(mesh):
    placed = (P("row", "col"),)
    return jax.shard_map(
        step, mesh=mesh, in_specs=placed, out_specs=P("row", ("layer", "col")), check_vma=False
    )
```

```python
import jax
import jax.numpy as jnp
from jax import lax
from jax.experimental import pallas as pl
from jax.experimental.pallas import tpu as pltpu
from jax.sharding import PartitionSpec as P


F32 = jnp.float32
BLOCKS = 8
THIRD = [
    [0, 3, 6, 4, 2, 7, 5, 1],
    [4, 1, 0, 5, 3, 6, 7, 2],
    [5, 6, 2, 1, 7, 4, 3, 0],
    [2, 7, 5, 3, 6, 0, 1, 4],
    [7, 5, 1, 2, 4, 3, 0, 6],
    [1, 2, 7, 6, 0, 5, 4, 3],
    [3, 0, 4, 7, 1, 2, 6, 5],
    [6, 4, 3, 0, 5, 1, 2, 7],
]
GRAM = {4: (0, 1), 5: (0, 2), 6: (0, 3), 7: (0, 3)}
PIECES = 4
ROWS_KIND, COLS_KIND, THIRD_KIND = 1, 2, 3
OWN_ROW, OWN_COL, OWN_DIAG, OWN_GRAM = 1, 2, 3, 4
CORES = 2


def node(r, c):
    return r * BLOCKS + c


def device(layer, r, c):
    return layer * BLOCKS * BLOCKS + node(r, c)


def plan():
    col_pairs, row_pairs, kinds = [], [], [[0, 0]] * (BLOCKS * BLOCKS)
    for r in range(BLOCKS):
        for c in range(BLOCKS):
            if r == c:
                continue
            m = THIRD[r][c]
            col_pairs.append((node(r, m), node(r, c)))
            row_pairs.append((node(m, c), node(r, c)))
            top = max(r, c, m)
            kinds[node(r, c)] = [{r: ROWS_KIND, c: COLS_KIND, m: THIRD_KIND}[top], top]
    diag_pairs, own = [[] for _ in range(PIECES)], [[0, 0]] * (BLOCKS**3)
    for d in range(BLOCKS):
        grams = GRAM.get(d, ())
        for layer in range(BLOCKS):
            own[device(layer, d, d)] = [OWN_GRAM if grams else OWN_DIAG, 0]
            for piece, o in enumerate(grams):
                diag_pairs[piece].append((device(layer, o, d), device(layer, d, d)))
        others = [o for o in range(BLOCKS) if o != d and o not in grams]
        for i, o in enumerate(others):
            for piece in range(PIECES):
                chip = CORES * ((piece + i) % PIECES)
                target = device(chip + (o < d), max(d, o), min(d, o))
                diag_pairs[piece].append((device(chip + i // PIECES, d, d), target))
                own[target] = [OWN_COL if o > d else OWN_ROW, piece]
    return col_pairs, row_pairs, diag_pairs, kinds, own


def mm(a, b, dims=((1,), (0,))):
    return lax.dot_general(a, b, (dims, ((), ())), preferred_element_type=F32)


def fold_lanes(w):
    part = w[:, :128]
    for t in range(1, w.shape[1] // 128):
        part = part + w[:, 128 * t : 128 * (t + 1)]
    return jnp.sum(part.T, axis=0, keepdims=True)


def fold_rows(w):
    return jnp.sum(w.reshape(w.shape[0] // 8, 8, w.shape[1]), axis=0)


STEP = 256


def triple_kernel(info_ref, b_ref, x_ref, z_ref, out_ref):
    here = lax.axis_index("row") * BLOCKS + lax.axis_index("col")
    kind, top, layer = info_ref[2 * here], info_ref[2 * here + 1], lax.axis_index("layer")
    n = b_ref.shape[0]
    out_ref[...] = jnp.zeros_like(out_ref)

    def put(vector, start):
        shape = (out_ref.shape[0], vector.shape[1])
        row = lax.broadcasted_iota(jnp.int32, shape, 0)
        spread = jnp.broadcast_to(vector, shape)
        out_ref[:, start : start + shape[1]] = jnp.where(row == top, spread, jnp.zeros_like(spread))

    @pl.when(kind == ROWS_KIND)
    def _():
        for s in range(0, n, STEP):
            w = mm(x_ref[s : s + STEP, :], z_ref[...]) * b_ref[s : s + STEP, :].astype(F32)
            put(fold_lanes(w), s)

    @pl.when(kind == COLS_KIND)
    def _():
        acc = jnp.zeros((8, n), F32)
        for s in range(0, n, STEP):
            w = mm(x_ref[s : s + STEP, :], z_ref[...]) * b_ref[s : s + STEP, :].astype(F32)
            acc = acc + fold_rows(w)
        put(jnp.sum(acc, axis=0, keepdims=True), 0)

    @pl.when(kind == THIRD_KIND)
    def _():
        width = x_ref.shape[1]
        acc = jnp.zeros((8, width), F32)
        for s in range(0, n, STEP):
            q = mm(b_ref[s : s + STEP, :], z_ref[...], ((1,), (1,)))
            acc = acc + fold_rows(q * x_ref[s : s + STEP, :].astype(F32))
        total = jnp.sum(acc, axis=0, keepdims=True)
        for k in range(n // width):
            @pl.when(layer == k)
            def _(k=k):
                put(total, k * width)


def own_kernel(info_ref, b_ref, *refs):
    u_refs, out_ref = refs[:-1], refs[-1]
    layer, r, c = (lax.axis_index(name) for name in ("layer", "row", "col"))
    here = (layer * BLOCKS + r) * BLOCKS + c
    own, piece, side = info_ref[2 * here], info_ref[2 * here + 1], r - c
    n = b_ref.shape[0]
    h = n // 2
    width = n // BLOCKS
    out_ref[...] = jnp.zeros_like(out_ref)

    def below(w, first_row):
        row = lax.broadcasted_iota(jnp.int32, w.shape, 0) + first_row
        col = lax.broadcasted_iota(jnp.int32, w.shape, 1)
        return jnp.where(row > col, w, jnp.zeros((), w.dtype))

    def parts(u_ref, first_row):
        mix = u_ref[:, h:]
        row = lax.broadcasted_iota(jnp.int32, mix.shape, 0) + first_row
        col = lax.broadcasted_iota(jnp.int32, mix.shape, 1)
        zero = jnp.zeros((), mix.dtype)
        return u_ref[:, :h], jnp.where(row < col, mix, zero), jnp.where(row > col, mix, zero)

    for k, u_ref in enumerate(u_refs):
        step = u_ref.shape[0]
        low, high = slice(k * step, (k + 1) * step), slice(h + k * step, h + (k + 1) * step)

        @pl.when(jnp.logical_and(own == OWN_COL, piece == k))
        def _(u_ref=u_ref, low=low, high=high, k=k, step=step):
            across, first, second = parts(u_ref, k * step)
            for s in range(0, n, STEP):
                cut = slice(s, s + STEP)
                lo, hi = b_ref[cut, low], b_ref[cut, high]
                p_lo = mm(hi, across) + mm(lo, first)
                w = p_lo * b_ref[cut, :h].astype(F32) + mm(hi, second) * b_ref[cut, h:].astype(F32)
                out_ref[0:1, cut] = fold_lanes(w)

        @pl.when(jnp.logical_and(own == OWN_ROW, piece == k))
        def _(u_ref=u_ref, low=low, high=high, k=k, step=step):
            across, first, second = parts(u_ref, k * step)
            for s in range(0, h, STEP):
                cut = slice(s, s + STEP)
                p = mm(first[:, cut], b_ref[low, :], ((0,), (0,)))
                out_ref[0:1, cut] = fold_lanes(p * b_ref[cut, :].astype(F32))
            p = mm(across, b_ref[:h, :]) + mm(second, b_ref[h:, :])
            out_ref[0:1, high] = fold_lanes(p * b_ref[high, :].astype(F32))

    for k in range(BLOCKS):
        cut = slice(k * width, (k + 1) * width)

        @pl.when(jnp.logical_and(layer == k, side >= 0))
        def _(cut=cut, k=k):
            rows = b_ref[cut, :]
            row = lax.broadcasted_iota(jnp.int32, rows.shape, 0) + k * width
            col = lax.broadcasted_iota(jnp.int32, rows.shape, 1)
            mine = jnp.logical_and(rows.astype(F32) > 0, jnp.logical_or(side > 0, row > col))
            out_ref[1:2, cut] = fold_lanes(jnp.where(mine, 1.0, 0.0).astype(F32))

        @pl.when(jnp.logical_and(layer == k, side == 0))
        def _(cut=cut, k=k):
            middle = below(b_ref[cut, :], k * width)
            for s in range(0, n, STEP):
                mine = below(b_ref[s : s + STEP, :], s)
                w = mm(mine[:, cut], middle) * mine.astype(F32)
                out_ref[0:1, s : s + STEP] = fold_lanes(w)


    for k in range(max(len(o) for o in GRAM.values())):
        @pl.when(own == OWN_GRAM)
        def _(u_ref=u_refs[k]):
            for s in range(0, n, STEP):
                e = s + STEP
                g = mm(u_ref[:, s:e], u_ref[:, :e], ((0,), (0,)))
                out_ref[0:1, s:e] += fold_lanes(g * below(b_ref[s:e, :e], s).astype(F32))


def cut_kernel(b_ref, columns_ref, rows_ref, sems):
    width = columns_ref.shape[1]
    start = pl.multiple_of(lax.axis_index("layer") * width, width)
    copies = (
        pltpu.make_async_copy(b_ref.at[:, pl.ds(start, width)], columns_ref, sems.at[0]),
        pltpu.make_async_copy(b_ref.at[pl.ds(start, width), :], rows_ref, sems.at[1]),
    )
    for copy in copies:
        copy.start()
    for copy in copies:
        copy.wait()


def pack_kernel(b_ref, rows_ref, *out_refs):
    h = b_ref.shape[0] // 2
    diagonal = lax.axis_index("row") == lax.axis_index("col")
    for k, out_ref in enumerate(out_refs):
        step = out_ref.shape[0]
        low, high = slice(k * step, (k + 1) * step), slice(h + k * step, h + (k + 1) * step)

        @pl.when(diagonal)
        def _(out_ref=out_ref, low=low, high=high, k=k, step=step):
            out_ref[:, :h] = b_ref[high, :h]
            row = lax.broadcasted_iota(jnp.int32, (step, h), 0) + k * step
            col = lax.broadcasted_iota(jnp.int32, (step, h), 1)
            out_ref[:, h:] = jnp.where(row > col, b_ref[high, h:], b_ref[low, :h])

        @pl.when(jnp.logical_not(diagonal))
        def _(out_ref=out_ref):
            out_ref[...] = rows_ref[...]


def cut(edge_weight):
    n = edge_weight.shape[0]
    width = n // BLOCKS
    return pl.pallas_call(
        cut_kernel,
        out_shape=(
            jax.ShapeDtypeStruct((n, width), edge_weight.dtype),
            jax.ShapeDtypeStruct((width, n), edge_weight.dtype),
        ),
        in_specs=[pl.BlockSpec(memory_space=pltpu.HBM)],
        out_specs=(pl.BlockSpec(memory_space=pltpu.VMEM), pl.BlockSpec(memory_space=pltpu.VMEM)),
        scratch_shapes=[pltpu.SemaphoreType.DMA((2,))],
        name="cut",
        cost_estimate=pl.CostEstimate(flops=0, bytes_accessed=4 * n * width, transcendentals=0),
        compiler_params=pltpu.CompilerParams(vmem_limit_bytes=8 * 1024 * 1024),
    )(edge_weight)


def pack(edge_weight, rows):
    n = edge_weight.shape[0]
    whole = pl.BlockSpec(memory_space=pltpu.VMEM)
    piece = jax.ShapeDtypeStruct((n // 2 // PIECES, n), edge_weight.dtype)
    return pl.pallas_call(
        pack_kernel,
        out_shape=(piece,) * PIECES,
        in_specs=[whole, whole],
        out_specs=(whole,) * PIECES,
        name="pack",
        cost_estimate=pl.CostEstimate(flops=0, bytes_accessed=2 * n * n, transcendentals=0),
        compiler_params=pltpu.CompilerParams(vmem_limit_bytes=16 * 1024 * 1024),
    )(edge_weight, rows)


def vmem_call(kernel, out_shape, flops, nbytes):
    whole = pl.BlockSpec(memory_space=pltpu.VMEM)

    def call(info, *arrays):
        return pl.pallas_call(
            kernel,
            out_shape=out_shape,
            in_specs=[pl.BlockSpec(memory_space=pltpu.SMEM)] + [whole] * len(arrays),
            out_specs=whole,
            cost_estimate=pl.CostEstimate(flops=flops, bytes_accessed=nbytes, transcendentals=0),
            compiler_params=pltpu.CompilerParams(vmem_limit_bytes=32 * 1024 * 1024),
        )(info, *arrays)

    return call


def step(edge_weight):
    n = edge_weight.shape[0]
    width = n // BLOCKS
    col_pairs, row_pairs, diag_pairs, kinds, own = plan()
    triple_info = jnp.array(kinds, jnp.int32).reshape(-1)
    own_info = jnp.array(own, jnp.int32).reshape(-1)

    columns, rows = cut(edge_weight)
    x = lax.ppermute(columns, ("row", "col"), col_pairs)
    z = lax.ppermute(rows, ("row", "col"), row_pairs)
    packed = pack(edge_weight, rows)
    u = [lax.ppermute(p, ("layer", "row", "col"), pairs) for p, pairs in zip(packed, diag_pairs)]

    triples = vmem_call(
        triple_kernel, jax.ShapeDtypeStruct((BLOCKS, n), F32), 2 * n * n * width, 2 * n * n
    )(triple_info, edge_weight, x, z)
    back = lax.all_to_all(triples, "row", 0, 0, tiled=True)
    mine = vmem_call(
        own_kernel, jax.ShapeDtypeStruct((2, n), F32), n * n * n // 2, 4 * n * n
    )(own_info, edge_weight, *u)
    total = jnp.sum(back, axis=0) + mine[0]
    peers = BLOCKS * BLOCKS
    sent = jnp.stack([total.reshape(peers, n // peers), mine[1].reshape(peers, n // peers)], axis=1)
    got = jnp.sum(lax.all_to_all(sent, ("layer", "col"), 0, 0, tiled=True), axis=0)
    degree = got[1]
    clustering = 2.0 * got[0] / jnp.maximum(degree * (degree - 1.0), 2.0)
    return clustering.reshape(1, -1)


def solution(mesh):
    placed = (P("row", "col"),)
    return jax.shard_map(
        step, mesh=mesh, in_specs=placed, out_specs=P("row", ("layer", "col")), check_vma=False
    )
```

```python
import jax
import jax.numpy as jnp
from jax import lax
from jax.experimental import pallas as pl
from jax.experimental.pallas import tpu as pltpu
from jax.sharding import PartitionSpec as P


F32 = jnp.float32
BLOCKS = 8
THIRD = [
    [0, 3, 6, 4, 2, 7, 5, 1],
    [4, 1, 0, 5, 3, 6, 7, 2],
    [5, 6, 2, 1, 7, 4, 3, 0],
    [2, 7, 5, 3, 6, 0, 1, 4],
    [7, 5, 1, 2, 4, 3, 0, 6],
    [1, 2, 7, 6, 0, 5, 4, 3],
    [3, 0, 4, 7, 1, 2, 6, 5],
    [6, 4, 3, 0, 5, 1, 2, 7],
]
GRAM = {4: (0, 1), 5: (0, 2), 6: (0, 3), 7: (0, 3)}
PIECES = 4
ROWS_KIND, COLS_KIND, THIRD_KIND = 1, 2, 3
OWN_ROW, OWN_COL, OWN_DIAG, OWN_GRAM = 1, 2, 3, 4
CORES = 2


def node(r, c):
    return r * BLOCKS + c


def device(layer, r, c):
    return layer * BLOCKS * BLOCKS + node(r, c)


def plan():
    col_pairs, row_pairs, kinds = [], [], [[0, 0]] * (BLOCKS * BLOCKS)
    for r in range(BLOCKS):
        for c in range(BLOCKS):
            if r == c:
                continue
            m = THIRD[r][c]
            col_pairs.append((node(r, m), node(r, c)))
            row_pairs.append((node(m, c), node(r, c)))
            top = max(r, c, m)
            kinds[node(r, c)] = [{r: ROWS_KIND, c: COLS_KIND, m: THIRD_KIND}[top], top]
    diag_pairs, own = [[] for _ in range(PIECES)], [[0, 0]] * (BLOCKS**3)
    for d in range(BLOCKS):
        grams = GRAM.get(d, ())
        for layer in range(BLOCKS):
            own[device(layer, d, d)] = [OWN_GRAM if grams else OWN_DIAG, 0]
            for piece, o in enumerate(grams):
                diag_pairs[piece].append((device(layer, o, d), device(layer, d, d)))
        others = [o for o in range(BLOCKS) if o != d and o not in grams]
        for i, o in enumerate(others):
            for piece in range(PIECES):
                chip = CORES * ((piece + i) % PIECES)
                target = device(chip + (o < d), max(d, o), min(d, o))
                diag_pairs[piece].append((device(chip + i // PIECES, d, d), target))
                own[target] = [OWN_COL if o > d else OWN_ROW, piece]
    return col_pairs, row_pairs, diag_pairs, kinds, own


def mm(a, b, dims=((1,), (0,))):
    return lax.dot_general(a, b, (dims, ((), ())), preferred_element_type=F32)


def fold_lanes(w):
    part = w[:, :128]
    for t in range(1, w.shape[1] // 128):
        part = part + w[:, 128 * t : 128 * (t + 1)]
    return jnp.sum(part.T, axis=0, keepdims=True)


def fold_rows(w):
    return jnp.sum(w.reshape(w.shape[0] // 8, 8, w.shape[1]), axis=0)


STEP = 256
LANES = 128


def triple_kernel(info_ref, b_ref, x_ref, z_ref, out_ref):
    here = lax.axis_index("row") * BLOCKS + lax.axis_index("col")
    kind, top, layer = info_ref[2 * here], info_ref[2 * here + 1], lax.axis_index("layer")
    n = b_ref.shape[0]
    out_ref[...] = jnp.zeros_like(out_ref)

    def put(vector, start):
        for t in range(vector.shape[1] // LANES):
            out_ref[top, start // LANES + t, :] = vector[0, t * LANES : (t + 1) * LANES]

    @pl.when(kind == ROWS_KIND)
    def _():
        for s in range(0, n, STEP):
            w = mm(x_ref[s : s + STEP, :], z_ref[...]) * b_ref[s : s + STEP, :].astype(F32)
            put(fold_lanes(w), s)

    @pl.when(kind == COLS_KIND)
    def _():
        acc = jnp.zeros((8, n), F32)
        for s in range(0, n, STEP):
            w = mm(x_ref[s : s + STEP, :], z_ref[...]) * b_ref[s : s + STEP, :].astype(F32)
            acc = acc + fold_rows(w)
        put(jnp.sum(acc, axis=0, keepdims=True), 0)

    @pl.when(kind == THIRD_KIND)
    def _():
        width = x_ref.shape[1]
        acc = jnp.zeros((8, width), F32)
        for s in range(0, n, STEP):
            q = mm(b_ref[s : s + STEP, :], z_ref[...], ((1,), (1,)))
            acc = acc + fold_rows(q * x_ref[s : s + STEP, :].astype(F32))
        total = jnp.sum(acc, axis=0, keepdims=True)
        for k in range(n // width):
            @pl.when(layer == k)
            def _(k=k):
                put(total, k * width)


def own_kernel(info_ref, b_ref, *refs):
    u_refs, out_ref = refs[:-1], refs[-1]
    layer, r, c = (lax.axis_index(name) for name in ("layer", "row", "col"))
    here = (layer * BLOCKS + r) * BLOCKS + c
    own, piece, side = info_ref[2 * here], info_ref[2 * here + 1], r - c
    n = b_ref.shape[0]
    h = n // 2
    width = n // BLOCKS
    out_ref[...] = jnp.zeros_like(out_ref)

    def below(w, first_row):
        row = lax.broadcasted_iota(jnp.int32, w.shape, 0) + first_row
        col = lax.broadcasted_iota(jnp.int32, w.shape, 1)
        return jnp.where(row > col, w, jnp.zeros((), w.dtype))

    def parts(u_ref, first_row):
        mix = u_ref[:, h:]
        row = lax.broadcasted_iota(jnp.int32, mix.shape, 0) + first_row
        col = lax.broadcasted_iota(jnp.int32, mix.shape, 1)
        zero = jnp.zeros((), mix.dtype)
        return u_ref[:, :h], jnp.where(row < col, mix, zero), jnp.where(row > col, mix, zero)

    for k, u_ref in enumerate(u_refs):
        step = u_ref.shape[0]
        low, high = slice(k * step, (k + 1) * step), slice(h + k * step, h + (k + 1) * step)

        @pl.when(jnp.logical_and(own == OWN_COL, piece == k))
        def _(u_ref=u_ref, low=low, high=high, k=k, step=step):
            across, first, second = parts(u_ref, k * step)
            for s in range(0, n, STEP):
                cut = slice(s, s + STEP)
                lo, hi = b_ref[cut, low], b_ref[cut, high]
                p_lo = mm(hi, across) + mm(lo, first)
                w = p_lo * b_ref[cut, :h].astype(F32) + mm(hi, second) * b_ref[cut, h:].astype(F32)
                out_ref[0:1, cut] = fold_lanes(w)

        @pl.when(jnp.logical_and(own == OWN_ROW, piece == k))
        def _(u_ref=u_ref, low=low, high=high, k=k, step=step):
            across, first, second = parts(u_ref, k * step)
            for s in range(0, h, STEP):
                cut = slice(s, s + STEP)
                p = mm(first[:, cut], b_ref[low, :], ((0,), (0,)))
                out_ref[0:1, cut] = fold_lanes(p * b_ref[cut, :].astype(F32))
            p = mm(across, b_ref[:h, :]) + mm(second, b_ref[h:, :])
            out_ref[0:1, high] = fold_lanes(p * b_ref[high, :].astype(F32))

    for k in range(BLOCKS):
        cut = slice(k * width, (k + 1) * width)

        @pl.when(jnp.logical_and(layer == k, side >= 0))
        def _(cut=cut, k=k):
            rows = b_ref[cut, :]
            row = lax.broadcasted_iota(jnp.int32, rows.shape, 0) + k * width
            col = lax.broadcasted_iota(jnp.int32, rows.shape, 1)
            mine = jnp.logical_and(rows.astype(F32) > 0, jnp.logical_or(side > 0, row > col))
            out_ref[1:2, cut] = fold_lanes(jnp.where(mine, 1.0, 0.0).astype(F32))

        @pl.when(jnp.logical_and(layer == k, side == 0))
        def _(cut=cut, k=k):
            middle = below(b_ref[cut, :], k * width)
            for s in range(0, n, STEP):
                mine = below(b_ref[s : s + STEP, :], s)
                w = mm(mine[:, cut], middle) * mine.astype(F32)
                out_ref[0:1, s : s + STEP] = fold_lanes(w)


    for k in range(max(len(o) for o in GRAM.values())):
        @pl.when(own == OWN_GRAM)
        def _(u_ref=u_refs[k]):
            for s in range(0, n, STEP):
                e = s + STEP
                g = mm(u_ref[:, s:e], u_ref[:, :e], ((0,), (0,)))
                out_ref[0:1, s:e] += fold_lanes(g * below(b_ref[s:e, :e], s).astype(F32))


def cut_kernel(b_ref, columns_ref, rows_ref, sems):
    width = columns_ref.shape[1]
    start = pl.multiple_of(lax.axis_index("layer") * width, width)
    copies = (
        pltpu.make_async_copy(b_ref.at[:, pl.ds(start, width)], columns_ref, sems.at[0]),
        pltpu.make_async_copy(b_ref.at[pl.ds(start, width), :], rows_ref, sems.at[1]),
    )
    for copy in copies:
        copy.start()
    for copy in copies:
        copy.wait()


def pack_kernel(b_ref, rows_ref, *out_refs):
    h = b_ref.shape[0] // 2
    diagonal = lax.axis_index("row") == lax.axis_index("col")
    for k, out_ref in enumerate(out_refs):
        step = out_ref.shape[0]
        low, high = slice(k * step, (k + 1) * step), slice(h + k * step, h + (k + 1) * step)

        @pl.when(diagonal)
        def _(out_ref=out_ref, low=low, high=high, k=k, step=step):
            out_ref[:, :h] = b_ref[high, :h]
            row = lax.broadcasted_iota(jnp.int32, (step, h), 0) + k * step
            col = lax.broadcasted_iota(jnp.int32, (step, h), 1)
            out_ref[:, h:] = jnp.where(row > col, b_ref[high, h:], b_ref[low, :h])

        @pl.when(jnp.logical_not(diagonal))
        def _(out_ref=out_ref):
            out_ref[...] = rows_ref[...]


def cut(edge_weight):
    n = edge_weight.shape[0]
    width = n // BLOCKS
    return pl.pallas_call(
        cut_kernel,
        out_shape=(
            jax.ShapeDtypeStruct((n, width), edge_weight.dtype),
            jax.ShapeDtypeStruct((width, n), edge_weight.dtype),
        ),
        in_specs=[pl.BlockSpec(memory_space=pltpu.HBM)],
        out_specs=(pl.BlockSpec(memory_space=pltpu.VMEM), pl.BlockSpec(memory_space=pltpu.VMEM)),
        scratch_shapes=[pltpu.SemaphoreType.DMA((2,))],
        name="cut",
        cost_estimate=pl.CostEstimate(flops=0, bytes_accessed=4 * n * width, transcendentals=0),
        compiler_params=pltpu.CompilerParams(vmem_limit_bytes=8 * 1024 * 1024),
    )(edge_weight)


def pack(edge_weight, rows):
    n = edge_weight.shape[0]
    whole = pl.BlockSpec(memory_space=pltpu.VMEM)
    piece = jax.ShapeDtypeStruct((n // 2 // PIECES, n), edge_weight.dtype)
    return pl.pallas_call(
        pack_kernel,
        out_shape=(piece,) * PIECES,
        in_specs=[whole, whole],
        out_specs=(whole,) * PIECES,
        name="pack",
        cost_estimate=pl.CostEstimate(flops=0, bytes_accessed=2 * n * n, transcendentals=0),
        compiler_params=pltpu.CompilerParams(vmem_limit_bytes=16 * 1024 * 1024),
    )(edge_weight, rows)


def vmem_call(kernel, out_shape, flops, nbytes):
    whole = pl.BlockSpec(memory_space=pltpu.VMEM)

    def call(info, *arrays):
        return pl.pallas_call(
            kernel,
            out_shape=out_shape,
            in_specs=[pl.BlockSpec(memory_space=pltpu.SMEM)] + [whole] * len(arrays),
            out_specs=whole,
            cost_estimate=pl.CostEstimate(flops=flops, bytes_accessed=nbytes, transcendentals=0),
            compiler_params=pltpu.CompilerParams(vmem_limit_bytes=32 * 1024 * 1024),
        )(info, *arrays)

    return call


def step(edge_weight):
    n = edge_weight.shape[0]
    width = n // BLOCKS
    col_pairs, row_pairs, diag_pairs, kinds, own = plan()
    triple_info = jnp.array(kinds, jnp.int32).reshape(-1)
    own_info = jnp.array(own, jnp.int32).reshape(-1)

    columns, rows = cut(edge_weight)
    x = lax.ppermute(columns, ("row", "col"), col_pairs)
    z = lax.ppermute(rows, ("row", "col"), row_pairs)
    packed = pack(edge_weight, rows)
    u = []
    for piece, pairs in enumerate(diag_pairs):
        u.append(lax.ppermute(packed[piece], ("layer", "row", "col"), pairs))

    triples = vmem_call(
        triple_kernel, jax.ShapeDtypeStruct((BLOCKS, n // LANES, LANES), F32), 2 * n * n * width, 2 * n * n
    )(triple_info, edge_weight, x, z)
    back = lax.all_to_all(triples, "row", 0, 0, tiled=True)
    mine = vmem_call(
        own_kernel, jax.ShapeDtypeStruct((2, n), F32), n * n * n // 2, 4 * n * n
    )(own_info, edge_weight, *u)
    total = jnp.sum(back, axis=0).reshape(n) + mine[0]
    peers = BLOCKS * BLOCKS
    sent = jnp.stack([total.reshape(peers, n // peers), mine[1].reshape(peers, n // peers)], axis=1)
    got = jnp.sum(lax.all_to_all(sent, ("layer", "col"), 0, 0, tiled=True), axis=0)
    degree = got[1]
    clustering = 2.0 * got[0] / jnp.maximum(degree * (degree - 1.0), 2.0)
    return clustering.reshape(1, -1)


def solution(mesh):
    placed = (P("row", "col"),)
    return jax.shard_map(
        step, mesh=mesh, in_specs=placed, out_specs=P("row", ("layer", "col")), check_vma=False
    )
```

```python
import jax
import jax.numpy as jnp
from jax import lax
from jax.experimental import pallas as pl
from jax.experimental.pallas import tpu as pltpu
from jax.sharding import PartitionSpec as P


F32 = jnp.float32
BLOCKS = 8
THIRD = [
    [0, 2, 6, 5, 3, 7, 4, 1],
    [3, 1, 7, 2, 6, 4, 0, 5],
    [5, 4, 2, 7, 0, 1, 3, 6],
    [2, 5, 4, 3, 1, 6, 7, 0],
    [1, 7, 5, 6, 4, 0, 2, 3],
    [6, 0, 3, 4, 7, 5, 1, 2],
    [7, 3, 1, 0, 5, 2, 6, 4],
    [4, 6, 0, 1, 2, 3, 5, 7],
]
GRAM = {4: (0, 3), 5: (0, 3), 6: (0, 3), 7: (0, 2)}
PIECES = 4
ROWS_KIND, COLS_KIND, THIRD_KIND = 1, 2, 3
OWN_ROW, OWN_COL, OWN_DIAG, OWN_GRAM = 1, 2, 3, 4
CORES = 2


def node(r, c):
    return r * BLOCKS + c


def device(layer, r, c):
    return layer * BLOCKS * BLOCKS + node(r, c)


def plan():
    col_pairs, row_pairs, kinds = [], [], [[0, 0]] * (BLOCKS * BLOCKS)
    for r in range(BLOCKS):
        for c in range(BLOCKS):
            if r == c:
                continue
            m = THIRD[r][c]
            col_pairs.append((node(r, m), node(r, c)))
            row_pairs.append((node(m, c), node(r, c)))
            top = max(r, c, m)
            kinds[node(r, c)] = [{r: ROWS_KIND, c: COLS_KIND, m: THIRD_KIND}[top], top]
    diag_pairs, own = [[] for _ in range(PIECES)], [[0, 0]] * (BLOCKS**3)
    for d in range(BLOCKS):
        grams = GRAM.get(d, ())
        for layer in range(BLOCKS):
            own[device(layer, d, d)] = [OWN_GRAM if grams else OWN_DIAG, 0]
            for piece, o in enumerate(grams):
                diag_pairs[piece].append((device(layer, o, d), device(layer, d, d)))
        others = [o for o in range(BLOCKS) if o != d and o not in grams]
        for i, o in enumerate(others):
            for piece in range(PIECES):
                chip = CORES * ((piece + i) % PIECES)
                target = device(chip + (o < d), max(d, o), min(d, o))
                diag_pairs[piece].append((device(chip + i // PIECES, d, d), target))
                own[target] = [OWN_COL if o > d else OWN_ROW, piece]
    return col_pairs, row_pairs, diag_pairs, kinds, own


def mm(a, b, dims=((1,), (0,))):
    return lax.dot_general(a, b, (dims, ((), ())), preferred_element_type=F32)


def fold_lanes(w):
    part = w[:, :128]
    for t in range(1, w.shape[1] // 128):
        part = part + w[:, 128 * t : 128 * (t + 1)]
    return jnp.sum(part.T, axis=0, keepdims=True)


def fold_rows(w):
    return jnp.sum(w.reshape(w.shape[0] // 8, 8, w.shape[1]), axis=0)


STEP = 256
LANES = 128


def triple_kernel(info_ref, b_ref, x_ref, z_ref, out_ref):
    here = lax.axis_index("row") * BLOCKS + lax.axis_index("col")
    kind, top, layer = info_ref[2 * here], info_ref[2 * here + 1], lax.axis_index("layer")
    n = b_ref.shape[0]
    out_ref[...] = jnp.zeros_like(out_ref)

    def put(vector, start):
        for t in range(vector.shape[1] // LANES):
            out_ref[top, start // LANES + t, :] = vector[0, t * LANES : (t + 1) * LANES]

    @pl.when(kind == ROWS_KIND)
    def _():
        for s in range(0, n, STEP):
            w = mm(x_ref[s : s + STEP, :], z_ref[...]) * b_ref[s : s + STEP, :].astype(F32)
            put(fold_lanes(w), s)

    @pl.when(kind == COLS_KIND)
    def _():
        acc = jnp.zeros((8, n), F32)
        for s in range(0, n, STEP):
            w = mm(x_ref[s : s + STEP, :], z_ref[...]) * b_ref[s : s + STEP, :].astype(F32)
            acc = acc + fold_rows(w)
        put(jnp.sum(acc, axis=0, keepdims=True), 0)

    @pl.when(kind == THIRD_KIND)
    def _():
        width = x_ref.shape[1]
        acc = jnp.zeros((8, width), F32)
        for s in range(0, n, STEP):
            q = mm(b_ref[s : s + STEP, :], z_ref[...], ((1,), (1,)))
            acc = acc + fold_rows(q * x_ref[s : s + STEP, :].astype(F32))
        total = jnp.sum(acc, axis=0, keepdims=True)
        for k in range(n // width):
            @pl.when(layer == k)
            def _(k=k):
                put(total, k * width)


def own_kernel(info_ref, b_ref, *refs):
    u_refs, out_ref = refs[:-1], refs[-1]
    layer, r, c = (lax.axis_index(name) for name in ("layer", "row", "col"))
    here = (layer * BLOCKS + r) * BLOCKS + c
    own, piece, side = info_ref[2 * here], info_ref[2 * here + 1], r - c
    n = b_ref.shape[0]
    h = n // 2
    width = n // BLOCKS
    out_ref[...] = jnp.zeros_like(out_ref)

    def below(w, first_row):
        row = lax.broadcasted_iota(jnp.int32, w.shape, 0) + first_row
        col = lax.broadcasted_iota(jnp.int32, w.shape, 1)
        return jnp.where(row > col, w, jnp.zeros((), w.dtype))

    def parts(u_ref, first_row):
        mix = u_ref[:, h:]
        row = lax.broadcasted_iota(jnp.int32, mix.shape, 0) + first_row
        col = lax.broadcasted_iota(jnp.int32, mix.shape, 1)
        zero = jnp.zeros((), mix.dtype)
        return u_ref[:, :h], jnp.where(row < col, mix, zero), jnp.where(row > col, mix, zero)

    for k, u_ref in enumerate(u_refs):
        step = u_ref.shape[0]
        low, high = slice(k * step, (k + 1) * step), slice(h + k * step, h + (k + 1) * step)

        @pl.when(jnp.logical_and(own == OWN_COL, piece == k))
        def _(u_ref=u_ref, low=low, high=high, k=k, step=step):
            across, first, second = parts(u_ref, k * step)
            for s in range(0, n, STEP):
                cut = slice(s, s + STEP)
                lo, hi = b_ref[cut, low], b_ref[cut, high]
                p_lo = mm(hi, across) + mm(lo, first)
                w = p_lo * b_ref[cut, :h].astype(F32) + mm(hi, second) * b_ref[cut, h:].astype(F32)
                out_ref[0:1, cut] = fold_lanes(w)

        @pl.when(jnp.logical_and(own == OWN_ROW, piece == k))
        def _(u_ref=u_ref, low=low, high=high, k=k, step=step):
            across, first, second = parts(u_ref, k * step)
            for s in range(0, h, STEP):
                cut = slice(s, s + STEP)
                p = mm(first[:, cut], b_ref[low, :], ((0,), (0,)))
                out_ref[0:1, cut] = fold_lanes(p * b_ref[cut, :].astype(F32))
            p = mm(across, b_ref[:h, :]) + mm(second, b_ref[h:, :])
            out_ref[0:1, high] = fold_lanes(p * b_ref[high, :].astype(F32))

    for k in range(BLOCKS):
        cut = slice(k * width, (k + 1) * width)

        @pl.when(jnp.logical_and(layer == k, side >= 0))
        def _(cut=cut, k=k):
            rows = b_ref[cut, :]
            row = lax.broadcasted_iota(jnp.int32, rows.shape, 0) + k * width
            col = lax.broadcasted_iota(jnp.int32, rows.shape, 1)
            mine = jnp.logical_and(rows.astype(F32) > 0, jnp.logical_or(side > 0, row > col))
            out_ref[1:2, cut] = fold_lanes(jnp.where(mine, 1.0, 0.0).astype(F32))

        @pl.when(jnp.logical_and(layer == k, side == 0))
        def _(cut=cut, k=k):
            middle = below(b_ref[cut, :], k * width)
            for s in range(0, n, STEP):
                mine = below(b_ref[s : s + STEP, :], s)
                w = mm(mine[:, cut], middle) * mine.astype(F32)
                out_ref[0:1, s : s + STEP] = fold_lanes(w)


    for k in range(max(len(o) for o in GRAM.values())):
        @pl.when(own == OWN_GRAM)
        def _(u_ref=u_refs[k]):
            for s in range(0, n, STEP):
                e = s + STEP
                g = mm(u_ref[:, s:e], u_ref[:, :e], ((0,), (0,)))
                out_ref[0:1, s:e] += fold_lanes(g * below(b_ref[s:e, :e], s).astype(F32))


def cut_kernel(b_ref, columns_ref, rows_ref, sems):
    width = columns_ref.shape[1]
    start = pl.multiple_of(lax.axis_index("layer") * width, width)
    copies = (
        pltpu.make_async_copy(b_ref.at[:, pl.ds(start, width)], columns_ref, sems.at[0]),
        pltpu.make_async_copy(b_ref.at[pl.ds(start, width), :], rows_ref, sems.at[1]),
    )
    for copy in copies:
        copy.start()
    for copy in copies:
        copy.wait()


def pack_kernel(b_ref, rows_ref, *out_refs):
    h = b_ref.shape[0] // 2
    diagonal = lax.axis_index("row") == lax.axis_index("col")
    for k, out_ref in enumerate(out_refs):
        step = out_ref.shape[0]
        low, high = slice(k * step, (k + 1) * step), slice(h + k * step, h + (k + 1) * step)

        @pl.when(diagonal)
        def _(out_ref=out_ref, low=low, high=high, k=k, step=step):
            out_ref[:, :h] = b_ref[high, :h]
            row = lax.broadcasted_iota(jnp.int32, (step, h), 0) + k * step
            col = lax.broadcasted_iota(jnp.int32, (step, h), 1)
            out_ref[:, h:] = jnp.where(row > col, b_ref[high, h:], b_ref[low, :h])

        @pl.when(jnp.logical_not(diagonal))
        def _(out_ref=out_ref):
            out_ref[...] = rows_ref[...]


def cut(edge_weight):
    n = edge_weight.shape[0]
    width = n // BLOCKS
    return pl.pallas_call(
        cut_kernel,
        out_shape=(
            jax.ShapeDtypeStruct((n, width), edge_weight.dtype),
            jax.ShapeDtypeStruct((width, n), edge_weight.dtype),
        ),
        in_specs=[pl.BlockSpec(memory_space=pltpu.HBM)],
        out_specs=(pl.BlockSpec(memory_space=pltpu.VMEM), pl.BlockSpec(memory_space=pltpu.VMEM)),
        scratch_shapes=[pltpu.SemaphoreType.DMA((2,))],
        name="cut",
        cost_estimate=pl.CostEstimate(flops=0, bytes_accessed=4 * n * width, transcendentals=0),
        compiler_params=pltpu.CompilerParams(vmem_limit_bytes=8 * 1024 * 1024),
    )(edge_weight)


def pack(edge_weight, rows):
    n = edge_weight.shape[0]
    whole = pl.BlockSpec(memory_space=pltpu.VMEM)
    piece = jax.ShapeDtypeStruct((n // 2 // PIECES, n), edge_weight.dtype)
    return pl.pallas_call(
        pack_kernel,
        out_shape=(piece,) * PIECES,
        in_specs=[whole, whole],
        out_specs=(whole,) * PIECES,
        name="pack",
        cost_estimate=pl.CostEstimate(flops=0, bytes_accessed=2 * n * n, transcendentals=0),
        compiler_params=pltpu.CompilerParams(vmem_limit_bytes=16 * 1024 * 1024),
    )(edge_weight, rows)


def vmem_call(kernel, out_shape, flops, nbytes):
    whole = pl.BlockSpec(memory_space=pltpu.VMEM)

    def call(info, *arrays):
        return pl.pallas_call(
            kernel,
            out_shape=out_shape,
            in_specs=[pl.BlockSpec(memory_space=pltpu.SMEM)] + [whole] * len(arrays),
            out_specs=whole,
            cost_estimate=pl.CostEstimate(flops=flops, bytes_accessed=nbytes, transcendentals=0),
            compiler_params=pltpu.CompilerParams(vmem_limit_bytes=32 * 1024 * 1024),
        )(info, *arrays)

    return call


def step(edge_weight):
    n = edge_weight.shape[0]
    width = n // BLOCKS
    col_pairs, row_pairs, diag_pairs, kinds, own = plan()
    triple_info = jnp.array(kinds, jnp.int32).reshape(-1)
    own_info = jnp.array(own, jnp.int32).reshape(-1)

    columns, rows = cut(edge_weight)
    x = lax.ppermute(columns, ("row", "col"), col_pairs)
    z = lax.ppermute(rows, ("row", "col"), row_pairs)
    packed = pack(edge_weight, rows)
    u = []
    for piece, pairs in enumerate(diag_pairs):
        u.append(lax.ppermute(packed[piece], ("layer", "row", "col"), pairs))

    triples = vmem_call(
        triple_kernel, jax.ShapeDtypeStruct((BLOCKS, n // LANES, LANES), F32), 2 * n * n * width, 2 * n * n
    )(triple_info, edge_weight, x, z)
    back = lax.all_to_all(triples, "row", 0, 0, tiled=True)
    mine = vmem_call(
        own_kernel, jax.ShapeDtypeStruct((2, n), F32), n * n * n // 2, 4 * n * n
    )(own_info, edge_weight, *u)
    total = jnp.sum(back, axis=0).reshape(n) + mine[0]
    peers = BLOCKS * BLOCKS
    sent = jnp.stack([total.reshape(peers, n // peers), mine[1].reshape(peers, n // peers)], axis=1)
    got = jnp.sum(lax.all_to_all(sent, ("layer", "col"), 0, 0, tiled=True), axis=0)
    degree = got[1]
    clustering = 2.0 * got[0] / jnp.maximum(degree * (degree - 1.0), 2.0)
    return clustering.reshape(1, -1)


def solution(mesh):
    placed = (P("row", "col"),)
    return jax.shard_map(
        step, mesh=mesh, in_specs=placed, out_specs=P("row", ("layer", "col")), check_vma=False
    )
```
